32 devices in a mesh: rep: 8 (over y, x, core), shard: 4 (over z).
Axes of the slice: x: 2, y: 2, z: 4, core: 2. Of those that a mesh axis runs over, the one named last changes fastest.
Arguments:
- deltas: bfloat16 [8, 512, 4096], P('rep', 'shard'), may hold values from -6 to 6
- presence: int32 [8], replicated, may hold values from 0 to 1, as said below
- owner_of: int32 [8], replicated, may hold values from 0 to 7, each once
- outer_params: float32 [512, 4096], P('shard', 'rep'), may hold values from -6 to 6
- momentum: float32 [512, 4096], P('shard', 'rep'), may hold values from -4 to 4
Outputs:
- new_weights: bfloat16 [512, 4096], P('shard')
- new_outer: float32 [512, 4096], P('shard', 'rep')
- new_momentum: float32 [512, 4096], P('shard', 'rep')
The draws below stay inside these ranges and needn't reach their ends.
Inputs may be any that keep to these rules, and one draw needn't show every extreme that they name: `presence`: at least one replica group is present.
All inputs are finite; a program needn't handle non-finite values.
Results may differ from the reference program's by a relative error of at most 0.0075.
Values may be sent and summed in bfloat16 or wider, within the bound.
A program may use at most 64 MiB of HBM per device.

```python
import jax
import jax.numpy as jnp
from jax import lax

D = 4096
ROWS = 512
REPS = 8
BLOCK = 512


def draw_presence(key, part):
    first = jax.random.fold_in(key, 11)
    second = jax.random.fold_in(key, 12)
    flags = jax.random.randint(first, (REPS,), 0, 2).astype(jnp.int32)
    chosen = jax.random.randint(second, (), 0, REPS)
    return flags.at[chosen].set(1).astype(jnp.int32)


def raised(drawn, own_key, source, target, shards_of, factor):
    owner, partner = [(jnp.arange(drawn.shape[dim]) // (drawn.shape[dim] // shards_of)).reshape([-1 if axis == dim else 1 for axis in range(drawn.ndim)]) for dim in (source, target)]
    chosen = jax.random.permutation(own_key, shards_of)[partner]
    strong = (owner == chosen) | (owner == (partner + shards_of // 2) % shards_of)
    return jnp.where(strong, factor * drawn, drawn)


def shard_levels(rng, shape, split, smallest, top_value):
    def one(axis_at, parts):
        draws = jax.random.uniform(jax.random.fold_in(jax.random.fold_in(rng, 6), axis_at), (parts,), jnp.float32, smallest / len(split), top_value / len(split))
        return jnp.repeat(jnp.exp(draws), shape[axis_at] // parts).reshape((-1,) + (1,) * (len(shape) - axis_at - 1))

    factor_of = one(*split[0])
    for cut in split[1:]:
        factor_of = factor_of * one(*cut)
    return factor_of


def gaussian(rng, extent, scale, bound, cuts=(), held_as=jnp.bfloat16):
    drawn = jax.random.normal(rng, extent, jnp.float32) * scale
    if len(cuts) > 0:
        drawn = shard_levels(rng, extent, cuts, -0.22, 0.18) * drawn
    return jnp.clip(drawn, min=-bound, max=bound).astype(held_as)


def bell_draw_with(own_key, extent, spread, bound, pieces, heavy, dtype=jnp.bfloat16):
    values = spread * jax.random.normal(own_key, extent, jnp.float32)
    if pieces:
        values = values * shard_levels(own_key, extent, pieces, -0.22, 0.18)
    return jnp.clip(raised(values, jax.random.fold_in(own_key, 3), *heavy), -bound, bound).astype(dtype)


def setup_inputs(seed: int = 0) -> dict:
    key_list = jax.random.split(jax.random.key(seed), 6)
    deltas = bell_draw_with(key_list[0], (REPS, ROWS, D), 1.0, 6.0, ((0, 8), (1, 4)), (0, 2, 8, 2.0))
    presence = draw_presence(jax.random.fold_in(key_list[5], 71), 0)
    owner_of = jax.random.permutation(key_list[2], REPS).astype(jnp.int32)
    outer_params = gaussian(key_list[3], (ROWS, D), 1.0, 6.0, ((0, 4), (1, 8)), jnp.float32)
    momentum = gaussian(key_list[4], (ROWS, D), 0.5, 4.0, ((0, 4), (1, 8)), jnp.float32)
    return {"deltas": deltas, "presence": presence, "owner_of": owner_of, "outer_params": outer_params, "momentum": momentum}


def reference(deltas, presence, owner_of, outer_params, momentum):
    present = presence.astype(jnp.float32)
    count = jnp.sum(present)

    def add_group(total, item):
        flag, delta = item
        return total + flag * delta.astype(jnp.float32), None

    start = jnp.zeros((ROWS, D), jnp.float32)
    total, unused = lax.scan(add_group, start, (present, deltas))
    average = total / count
    blocks = average.reshape(ROWS, REPS, BLOCK)
    slotted = jnp.take(blocks, owner_of.astype(jnp.int32), axis=1).reshape(ROWS, D)
    new_momentum = 0.9 * momentum + slotted
    new_outer = outer_params - 0.7 * (slotted + 0.9 * new_momentum)
    inverse = jnp.argsort(owner_of).astype(jnp.int32)
    natural = jnp.take(new_outer.reshape(ROWS, REPS, BLOCK), inverse, axis=1).reshape(ROWS, D)
    new_weights = natural.astype(jnp.bfloat16)
    return (new_weights, new_outer, new_momentum)
```

```python
import functools

import jax
import jax.numpy as jnp
from jax import lax
from jax.experimental import pallas as pl
from jax.experimental.pallas import tpu as pltpu
from jax.sharding import PartitionSpec as P

MESH = pl.DeviceIdType.MESH


def toggled(index, mask, size):
    out, bit = 0, 1
    while bit < size:
        digit = (index // bit) % 2
        out = out + bit * ((1 - digit) if mask & bit else digit)
        bit *= 2
    return out


def exchange(n, chunks, presence, owner_of, deltas, outer_params, momentum, gathered, average,
             held_low, held_high, params, speed, out0, in0, out1, own, in1,
             load_sem, state_sem, send0, recv0, send1, recv1, send2, recv2, send3, recv3):
    me = lax.axis_index("rep")
    side, team = me % 2, me // 2
    partner = me + 1 - 2 * side
    teams = n // 2
    rows, width = average.shape
    part = rows // chunks
    mates = [toggled(team, d, teams) for d in range(teams)]
    peers = [2 * mate + side for mate in mates]
    order = list(range(teams - 1, 0, -1))

    def span(k):
        return pl.ds(k * part, part)

    def remote(src, dst, send, recv, to):
        return pltpu.make_async_remote_copy(
            src_ref=src, dst_ref=dst, send_sem=send, recv_sem=recv, device_id={"rep": to}, device_id_type=MESH)

    barrier = pltpu.get_barrier_semaphore()
    for to in [partner] + [peers[d] for d in order]:
        pl.semaphore_signal(barrier, inc=1, device_id={"rep": to}, device_id_type=MESH)

    held = (held_low, held_high)
    pieces, tall = len(held), rows // len(held)
    loads = [[pltpu.make_async_copy(deltas.at[0, pl.ds(i * tall, tall), pl.ds(j * width, width)],
                                    held[i].at[j], load_sem.at[i, j]) for j in range(n)]
             for i in range(pieces)]
    for load in sum(loads, []):
        load.start()
    state = [pltpu.make_async_copy(outer_params, params, state_sem.at[0]),
             pltpu.make_async_copy(momentum, speed, state_sem.at[1])]
    for load in state:
        load.start()

    flag = presence[me].astype(jnp.float32)
    count = presence[0].astype(jnp.float32)
    for r in range(1, n):
        count = count + presence[r].astype(jnp.float32)
    share = jnp.full((1, width), 1.0, jnp.float32) / jnp.full((1, width), count, jnp.float32)

    def term(k, slot):
        piece, first = divmod(k * part, tall)
        return held[piece][owner_of[slot], pl.ds(first, part)].astype(jnp.float32) * flag

    pending = []
    for k in range(chunks):
        if (k * part) % tall == 0:
            for load in loads[k * part // tall]:
                load.wait()
        for d in range(teams):
            out0[k, d] = term(k, 2 * mates[d] + 1 - side).astype(jnp.bfloat16)
        if k == 0:
            pl.semaphore_wait(barrier, teams)
        copy = remote(out0.at[k], in0.at[k], send0.at[k], recv0.at[k], partner)
        copy.start()
        pending.append(copy)
    firsts = list(pending)

    seconds = {}
    for k in range(chunks):
        firsts[k].wait_recv()
        for d in order:
            total = term(k, peers[d]) + in0[k, d].astype(jnp.float32)
            out1[k, d - 1] = total.astype(jnp.bfloat16)
            copy = remote(out1.at[k, d - 1], in1.at[k, d - 1], send1.at[k, d - 1], recv1.at[k, d - 1], peers[d])
            copy.start()
            seconds[k, d] = copy
            pending.append(copy)
        own[span(k)] = term(k, peers[0]) + in0[k, 0].astype(jnp.float32)

    for load in state:
        load.wait()
    thirds, fourths = {}, []
    for k in range(chunks):
        total = own[span(k)]
        for d in order:
            seconds[k, d].wait_recv()
            total = total + in1[k, d - 1].astype(jnp.float32)
        mean = total * share
        average[span(k)] = mean
        new_momentum = 0.9 * speed[span(k)] + mean
        new_outer = params[span(k)] - 0.7 * (mean + 0.9 * new_momentum)
        gathered[me, span(k)] = new_outer.astype(jnp.bfloat16)
        block = gathered.at[me, span(k)]
        for d in order:
            copy = remote(block, block, send2.at[k, d - 1], recv2.at[k, d - 1], peers[d])
            copy.start()
            thirds[k, d] = copy
            pending.append(copy)
        copy = remote(block, block, send3.at[k, 0], recv3.at[k, 0], partner)
        copy.start()
        fourths.append(copy)

    for k in range(chunks):
        for d in order[::-1]:
            thirds[k, d].wait_recv()
            block = gathered.at[peers[d], span(k)]
            copy = remote(block, block, send3.at[k, d], recv3.at[k, d], partner)
            copy.start()
            fourths.append(copy)
    for copy in fourths:
        copy.wait_recv()
    for copy in pending + fourths:
        copy.wait_send()


def finish(n, owner_of, gathered, average, outer_params, momentum, new_weights, new_outer, new_momentum,
           outer_out, momentum_out, block_sem, state_sem):
    width = gathered.shape[2]
    copies = []
    for j in range(n):
        start = pl.multiple_of(owner_of[j] * width, width)
        copies.append(pltpu.make_async_copy(gathered.at[j], new_weights.at[:, pl.ds(start, width)], block_sem.at[j]))
    for copy in copies:
        copy.start()
    mean = average[...]
    speed = 0.9 * momentum[...] + mean
    momentum_out[...] = speed
    outer_out[...] = outer_params[...] - 0.7 * (mean + 0.9 * speed)
    last = [pltpu.make_async_copy(momentum_out, new_momentum, state_sem.at[0]),
            pltpu.make_async_copy(outer_out, new_outer, state_sem.at[1])]
    for copy in last:
        copy.start()
    for copy in copies + last:
        copy.wait()


def shards(deltas, presence, owner_of, outer_params, momentum):
    n = lax.axis_size("rep")
    teams = n // 2
    rows, width = outer_params.shape
    chunks = 4
    part = rows // chunks
    bf16, f32 = jnp.bfloat16, jnp.float32
    smem = pl.BlockSpec(memory_space=pltpu.SMEM)
    vmem = pl.BlockSpec(memory_space=pltpu.VMEM)
    anywhere = pl.BlockSpec(memory_space=pl.ANY)
    hbm = pl.BlockSpec(memory_space=pltpu.HBM)
    dma = pltpu.SemaphoreType.DMA
    gathered, average = pl.pallas_call(
        functools.partial(exchange, n, chunks),
        out_shape=(jax.ShapeDtypeStruct((n, rows, width), bf16), jax.ShapeDtypeStruct((rows, width), f32)),
        in_specs=[smem, smem, hbm, hbm, hbm],
        out_specs=(vmem, vmem),
        scratch_shapes=[
            pltpu.VMEM((n, rows // 2, width), bf16),
            pltpu.VMEM((n, rows // 2, width), bf16),
            pltpu.VMEM((rows, width), f32),
            pltpu.VMEM((rows, width), f32),
            pltpu.VMEM((chunks, teams, part, width), bf16),
            pltpu.VMEM((chunks, teams, part, width), bf16),
            pltpu.VMEM((chunks, teams - 1, part, width), bf16),
            pltpu.VMEM((rows, width), f32),
            pltpu.VMEM((chunks, teams - 1, part, width), bf16),
            dma((2, n)), dma((2,)),
            dma((chunks,)), dma((chunks,)),
            dma((chunks, teams - 1)), dma((chunks, teams - 1)),
            dma((chunks, teams - 1)), dma((chunks, teams - 1)),
            dma((chunks, teams)), dma((chunks, teams)),
        ],
        compiler_params=pltpu.CompilerParams(collective_id=0, has_side_effects=True, vmem_limit_bytes=12 << 20),
        name="exchange",
    )(presence, owner_of, deltas, outer_params, momentum)
    return pl.pallas_call(
        functools.partial(finish, n),
        out_shape=(
            jax.ShapeDtypeStruct((rows, n * width), bf16),
            jax.ShapeDtypeStruct((rows, width), f32),
            jax.ShapeDtypeStruct((rows, width), f32),
        ),
        in_specs=[smem, vmem, vmem, vmem, vmem],
        out_specs=(anywhere, anywhere, anywhere),
        scratch_shapes=[
            pltpu.VMEM((rows, width), f32),
            pltpu.VMEM((rows, width), f32),
            dma((n,)), dma((2,)),
        ],
        compiler_params=pltpu.CompilerParams(vmem_limit_bytes=8 << 20),
        name="finish",
    )(owner_of, gathered, average, outer_params, momentum)


def solution(mesh):
    return jax.shard_map(
        shards,
        mesh=mesh,
        in_specs=(P("rep", "shard", None), P(), P(), P("shard", "rep"), P("shard", "rep")),
        out_specs=(P("shard", None), P("shard", "rep"), P("shard", "rep")),
        check_vma=False,
    )
```

```python
import functools

import jax
import jax.numpy as jnp
from jax import lax
from jax.experimental import pallas as pl
from jax.experimental.pallas import tpu as pltpu
from jax.sharding import PartitionSpec as P

MESH = pl.DeviceIdType.MESH


def toggled(index, mask, size):
    out, bit = 0, 1
    while bit < size:
        digit = (index // bit) % 2
        out = out + bit * ((1 - digit) if mask & bit else digit)
        bit *= 2
    return out


def exchange(n, chunks, presence, owner_of, deltas, outer_params, momentum, gathered, outer_out, momentum_out,
             held_low, held_high, params, speed, out0, in0, out1, own, in1,
             load_sem, state_sem, send0, recv0, send1, recv1, send2, recv2, send3, recv3):
    me = lax.axis_index("rep")
    side, team = me % 2, me // 2
    partner = me + 1 - 2 * side
    teams = n // 2
    rows, width = outer_out.shape
    part = rows // chunks
    mates = [toggled(team, d, teams) for d in range(teams)]
    peers = [2 * mate + side for mate in mates]
    order = list(range(teams - 1, 0, -1))

    def span(k):
        return pl.ds(k * part, part)

    def remote(src, dst, send, recv, to):
        return pltpu.make_async_remote_copy(
            src_ref=src, dst_ref=dst, send_sem=send, recv_sem=recv, device_id={"rep": to}, device_id_type=MESH)

    barrier = pltpu.get_barrier_semaphore()
    for to in [partner] + [peers[d] for d in order]:
        pl.semaphore_signal(barrier, inc=1, device_id={"rep": to}, device_id_type=MESH)

    held = (held_low, held_high)
    pieces, tall = len(held), rows // len(held)
    loads = [[pltpu.make_async_copy(deltas.at[0, pl.ds(i * tall, tall), pl.ds(j * width, width)],
                                    held[i].at[j], load_sem.at[i, j]) for j in range(n)]
             for i in range(pieces)]
    for load in sum(loads, []):
        load.start()
    state = [pltpu.make_async_copy(outer_params, params, state_sem.at[0]),
             pltpu.make_async_copy(momentum, speed, state_sem.at[1])]
    for load in state:
        load.start()

    flag = presence[me].astype(jnp.float32)
    count = presence[0].astype(jnp.float32)
    for r in range(1, n):
        count = count + presence[r].astype(jnp.float32)
    share = jnp.full((1, width), 1.0, jnp.float32) / jnp.full((1, width), count, jnp.float32)

    def term(k, slot):
        piece, first = divmod(k * part, tall)
        return held[piece][owner_of[slot], pl.ds(first, part)].astype(jnp.float32) * flag

    pending = []
    for k in range(chunks):
        if (k * part) % tall == 0:
            for load in loads[k * part // tall]:
                load.wait()
        for d in range(teams):
            out0[k, d] = term(k, 2 * mates[d] + 1 - side).astype(jnp.bfloat16)
        if k == 0:
            pl.semaphore_wait(barrier, teams)
        copy = remote(out0.at[k], in0.at[k], send0.at[k], recv0.at[k], partner)
        copy.start()
        pending.append(copy)
    firsts = list(pending)

    seconds = {}
    for k in range(chunks):
        firsts[k].wait_recv()
        for d in order:
            total = term(k, peers[d]) + in0[k, d].astype(jnp.float32)
            out1[k, d - 1] = total.astype(jnp.bfloat16)
            copy = remote(out1.at[k, d - 1], in1.at[k, d - 1], send1.at[k, d - 1], recv1.at[k, d - 1], peers[d])
            copy.start()
            seconds[k, d] = copy
            pending.append(copy)
        own[span(k)] = term(k, peers[0]) + in0[k, 0].astype(jnp.float32)

    for load in state:
        load.wait()
    thirds, fourths = {}, []
    for k in range(chunks):
        total = own[span(k)]
        for d in order:
            seconds[k, d].wait_recv()
            total = total + in1[k, d - 1].astype(jnp.float32)
        mean = total * share
        new_momentum = 0.9 * speed[span(k)] + mean
        new_outer = params[span(k)] - 0.7 * (mean + 0.9 * new_momentum)
        momentum_out[span(k)] = new_momentum
        outer_out[span(k)] = new_outer
        gathered[me, span(k)] = new_outer.astype(jnp.bfloat16)
        block = gathered.at[me, span(k)]
        for d in order:
            copy = remote(block, block, send2.at[k, d - 1], recv2.at[k, d - 1], peers[d])
            copy.start()
            thirds[k, d] = copy
            pending.append(copy)
        copy = remote(block, block, send3.at[k, 0], recv3.at[k, 0], partner)
        copy.start()
        fourths.append(copy)

    for k in range(chunks):
        for d in order[::-1]:
            thirds[k, d].wait_recv()
            block = gathered.at[peers[d], span(k)]
            copy = remote(block, block, send3.at[k, d], recv3.at[k, d], partner)
            copy.start()
            fourths.append(copy)
    for copy in fourths:
        copy.wait_recv()
    for copy in pending + fourths:
        copy.wait_send()


def finish(n, owner_of, gathered, outer, speed, new_weights, new_outer, new_momentum, block_sem, state_sem):
    width = gathered.shape[2]
    copies = []
    for j in range(n):
        start = pl.multiple_of(owner_of[j] * width, width)
        copies.append(pltpu.make_async_copy(gathered.at[j], new_weights.at[:, pl.ds(start, width)], block_sem.at[j]))
    copies += [pltpu.make_async_copy(outer, new_outer, state_sem.at[0]),
               pltpu.make_async_copy(speed, new_momentum, state_sem.at[1])]
    for copy in copies:
        copy.start()
    for copy in copies:
        copy.wait()


def shards(deltas, presence, owner_of, outer_params, momentum):
    n = lax.axis_size("rep")
    teams = n // 2
    rows, width = outer_params.shape
    chunks = 4
    part = rows // chunks
    bf16, f32 = jnp.bfloat16, jnp.float32
    smem = pl.BlockSpec(memory_space=pltpu.SMEM)
    vmem = pl.BlockSpec(memory_space=pltpu.VMEM)
    anywhere = pl.BlockSpec(memory_space=pl.ANY)
    hbm = pl.BlockSpec(memory_space=pltpu.HBM)
    dma = pltpu.SemaphoreType.DMA
    here = functools.partial(pltpu.with_memory_space_constraint, memory_space=pltpu.HBM)
    owner_of = here(owner_of)
    gathered, outer, speed = pl.pallas_call(
        functools.partial(exchange, n, chunks),
        out_shape=(pltpu.VMEM((n, rows, width), bf16), pltpu.VMEM((rows, width), f32), pltpu.VMEM((rows, width), f32)),
        in_specs=[smem, smem, hbm, hbm, hbm],
        out_specs=(vmem, vmem, vmem),
        scratch_shapes=[
            pltpu.VMEM((n, rows // 2, width), bf16),
            pltpu.VMEM((n, rows // 2, width), bf16),
            pltpu.VMEM((rows, width), f32),
            pltpu.VMEM((rows, width), f32),
            pltpu.VMEM((chunks, teams, part, width), bf16),
            pltpu.VMEM((chunks, teams, part, width), bf16),
            pltpu.VMEM((chunks, teams - 1, part, width), bf16),
            pltpu.VMEM((rows, width), f32),
            pltpu.VMEM((chunks, teams - 1, part, width), bf16),
            dma((2, n)), dma((2,)),
            dma((chunks,)), dma((chunks,)),
            dma((chunks, teams - 1)), dma((chunks, teams - 1)),
            dma((chunks, teams - 1)), dma((chunks, teams - 1)),
            dma((chunks, teams)), dma((chunks, teams)),
        ],
        compiler_params=pltpu.CompilerParams(collective_id=0, has_side_effects=True, vmem_limit_bytes=12 << 20),
        name="exchange",
    )(here(presence), owner_of, here(deltas), here(outer_params), here(momentum))
    return pl.pallas_call(
        functools.partial(finish, n),
        out_shape=(
            jax.ShapeDtypeStruct((rows, n * width), bf16),
            jax.ShapeDtypeStruct((rows, width), f32),
            jax.ShapeDtypeStruct((rows, width), f32),
        ),
        in_specs=[smem, vmem, vmem, vmem],
        out_specs=(anywhere, anywhere, anywhere),
        scratch_shapes=[dma((n,)), dma((2,))],
        compiler_params=pltpu.CompilerParams(vmem_limit_bytes=8 << 20),
        name="finish",
    )(owner_of, gathered, outer, speed)


def solution(mesh):
    return jax.shard_map(
        shards,
        mesh=mesh,
        in_specs=(P("rep", "shard", None), P(), P(), P("shard", "rep"), P("shard", "rep")),
        out_specs=(P("shard", None), P("shard", "rep"), P("shard", "rep")),
        check_vma=False,
    )
```

```python
import functools

import jax
import jax.numpy as jnp
from jax import lax
from jax.experimental import pallas as pl
from jax.experimental.pallas import tpu as pltpu
from jax.sharding import PartitionSpec as P

MESH = pl.DeviceIdType.MESH


def toggled(index, mask, size):
    out, bit = 0, 1
    while bit < size:
        digit = (index // bit) % 2
        out = out + bit * ((1 - digit) if mask & bit else digit)
        bit *= 2
    return out


def exchange(n, chunks, presence, owner_of, deltas, outer_params, momentum, gathered, outer_out, momentum_out,
             held_low, held_high, params, speed, out0, in0, out1, in1, out2, in2, own,
             load_sem, state_sem, send0, recv0, send1, recv1, send2, recv2, send3, recv3, send4, recv4):
    me = lax.axis_index("rep")
    side, team = me % 2, me // 2
    partner = me + 1 - 2 * side
    teams = n // 2
    rows, width = outer_out.shape
    part = rows // chunks
    mates = [toggled(team, d, teams) for d in range(teams)]
    peers = [2 * mate + side for mate in mates]
    order = list(range(teams - 1, 0, -1))

    def span(k):
        return pl.ds(k * part, part)

    def remote(src, dst, send, recv, to):
        return pltpu.make_async_remote_copy(
            src_ref=src, dst_ref=dst, send_sem=send, recv_sem=recv, device_id={"rep": to}, device_id_type=MESH)

    barrier = pltpu.get_barrier_semaphore()
    for to in [partner] + [peers[d] for d in order]:
        pl.semaphore_signal(barrier, inc=1, device_id={"rep": to}, device_id_type=MESH)

    held = (held_low, held_high)
    pieces, tall = len(held), rows // len(held)
    loads = [[pltpu.make_async_copy(deltas.at[0, pl.ds(i * tall, tall), pl.ds(j * width, width)],
                                    held[i].at[j], load_sem.at[i, j]) for j in range(n)]
             for i in range(pieces)]
    for load in sum(loads, []):
        load.start()
    state = [pltpu.make_async_copy(outer_params, params, state_sem.at[0]),
             pltpu.make_async_copy(momentum, speed, state_sem.at[1])]
    for load in state:
        load.start()

    flag = presence[me].astype(jnp.float32)
    count = presence[0].astype(jnp.float32)
    for r in range(1, n):
        count = count + presence[r].astype(jnp.float32)
    share = jnp.full((1, width), 1.0, jnp.float32) / jnp.full((1, width), count, jnp.float32)

    def term(k, slot):
        piece, first = divmod(k * part, tall)
        return held[piece][owner_of[slot], pl.ds(first, part)].astype(jnp.float32) * flag

    pending = []
    for k in range(chunks):
        if (k * part) % tall == 0:
            for load in loads[k * part // tall]:
                load.wait()
        for d in range(teams):
            out0[k, d] = term(k, 2 * mates[d] + 1 - side).astype(jnp.bfloat16)
        if k == 0:
            pl.semaphore_wait(barrier, teams)
        copy = remote(out0.at[k], in0.at[k], send0.at[k], recv0.at[k], partner)
        copy.start()
        pending.append(copy)
    firsts = list(pending)

    low = 1
    while low * low * 4 <= teams:
        low *= 2
    plans = []
    for k in range(chunks):
        steps = (1, low) if k % 2 == 0 else (low, 1)
        sizes = (low, teams // low) if k % 2 == 0 else (teams // low, low)
        plans.append((sizes, lambda f, s, steps=steps: f * steps[0] + s * steps[1]))

    def pair_sum(k, d):
        return term(k, peers[d]) + in0[k, d].astype(jnp.float32)

    seconds = {}
    for k in range(chunks):
        (first, second), mask = plans[k]
        firsts[k].wait_recv()
        for f in range(1, first):
            for s in range(second):
                out1[k, (f - 1) * second + s] = pair_sum(k, mask(f, s)).astype(jnp.bfloat16)
            bundle = pl.ds((f - 1) * second, second)
            copy = remote(out1.at[k, bundle], in1.at[k, bundle], send1.at[k, f - 1], recv1.at[k, f - 1],
                          peers[mask(f, 0)])
            copy.start()
            seconds[k, f] = copy
            pending.append(copy)

    thirds = {}
    for k in range(chunks):
        (first, second), mask = plans[k]
        for f in range(1, first):
            seconds[k, f].wait_recv()
        for s in list(range(1, second)) + [0]:
            total = pair_sum(k, mask(0, s))
            for f in range(1, first):
                total = total + in1[k, (f - 1) * second + s].astype(jnp.float32)
            if s == 0:
                own[span(k)] = total
                continue
            out2[k, s - 1] = total.astype(jnp.bfloat16)
            copy = remote(out2.at[k, s - 1], in2.at[k, s - 1], send2.at[k, s - 1], recv2.at[k, s - 1],
                          peers[mask(0, s)])
            copy.start()
            thirds[k, s] = copy
            pending.append(copy)

    for load in state:
        load.wait()
    arrivals, handed = {}, []

    def ship(k, origin, via):
        block, d = gathered.at[peers[origin], span(k)], origin + via
        arrivals[k, d] = remote(block, block, send3.at[k, d - 1], recv3.at[k, d - 1], peers[via])
        arrivals[k, d].start()
        pending.append(arrivals[k, d])

    def hand(k, d):
        block = gathered.at[peers[d], span(k)]
        copy = remote(block, block, send4.at[k, d], recv4.at[k, d], partner)
        copy.start()
        handed.append(copy)

    def update(k):
        (first, second), mask = plans[k]
        total = own[span(k)]
        for s in range(1, second):
            thirds[k, s].wait_recv()
            total = total + in2[k, s - 1].astype(jnp.float32)
        mean = total * share
        new_momentum = 0.9 * speed[span(k)] + mean
        new_outer = params[span(k)] - 0.7 * (mean + 0.9 * new_momentum)
        gathered[me, span(k)] = new_outer.astype(jnp.bfloat16)
        for f in range(1, first):
            ship(k, 0, mask(f, 0))
        for s in range(1, second):
            ship(k, 0, mask(0, s))
        hand(k, 0)
        momentum_out[span(k)] = new_momentum
        outer_out[span(k)] = new_outer

    def relay(k):
        (first, second), mask = plans[k]
        for f in range(1, first):
            arrivals[k, mask(f, 0)].wait_recv()
            for s in range(1, second):
                ship(k, mask(f, 0), mask(0, s))
            hand(k, mask(f, 0))

    def settle(k):
        (first, second), mask = plans[k]
        for s in range(1, second):
            for f in range(first):
                arrivals[k, mask(f, s)].wait_recv()
                hand(k, mask(f, s))

    lag = min(2, chunks)
    for k in range(chunks + lag):
        if k < chunks:
            update(k)
        if k >= lag:
            relay(k - lag)
    for k in range(chunks):
        settle(k)
    for copy in handed:
        copy.wait_recv()
    for copy in pending + handed:
        copy.wait_send()


def finish(n, owner_of, gathered, outer, speed, new_weights, new_outer, new_momentum, block_sem, state_sem):
    width = gathered.shape[2]
    copies = []
    for j in range(n):
        start = pl.multiple_of(owner_of[j] * width, width)
        copies.append(pltpu.make_async_copy(gathered.at[j], new_weights.at[:, pl.ds(start, width)], block_sem.at[j]))
    copies += [pltpu.make_async_copy(outer, new_outer, state_sem.at[0]),
               pltpu.make_async_copy(speed, new_momentum, state_sem.at[1])]
    for copy in copies:
        copy.start()
    for copy in copies:
        copy.wait()


def shards(deltas, presence, owner_of, outer_params, momentum):
    n = lax.axis_size("rep")
    teams = n // 2
    rows, width = outer_params.shape
    chunks = 4
    part = rows // chunks
    bf16, f32 = jnp.bfloat16, jnp.float32
    smem = pl.BlockSpec(memory_space=pltpu.SMEM)
    vmem = pl.BlockSpec(memory_space=pltpu.VMEM)
    anywhere = pl.BlockSpec(memory_space=pl.ANY)
    hbm = pl.BlockSpec(memory_space=pltpu.HBM)
    dma = pltpu.SemaphoreType.DMA
    here = functools.partial(pltpu.with_memory_space_constraint, memory_space=pltpu.HBM)
    owner_of = here(owner_of)
    gathered, outer, speed = pl.pallas_call(
        functools.partial(exchange, n, chunks),
        out_shape=(pltpu.VMEM((n, rows, width), bf16), pltpu.VMEM((rows, width), f32), pltpu.VMEM((rows, width), f32)),
        in_specs=[smem, smem, hbm, hbm, hbm],
        out_specs=(vmem, vmem, vmem),
        scratch_shapes=[
            pltpu.VMEM((n, rows // 2, width), bf16),
            pltpu.VMEM((n, rows // 2, width), bf16),
            pltpu.VMEM((rows, width), f32),
            pltpu.VMEM((rows, width), f32),
            pltpu.VMEM((chunks, teams, part, width), bf16),
            pltpu.VMEM((chunks, teams, part, width), bf16),
            pltpu.VMEM((chunks, teams - 1, part, width), bf16),
            pltpu.VMEM((chunks, teams - 1, part, width), bf16),
            pltpu.VMEM((chunks, teams - 1, part, width), bf16),
            pltpu.VMEM((chunks, teams - 1, part, width), bf16),
            pltpu.VMEM((rows, width), f32),
            dma((2, n)), dma((2,)),
            dma((chunks,)), dma((chunks,)),
            dma((chunks, teams - 1)), dma((chunks, teams - 1)),
            dma((chunks, teams - 1)), dma((chunks, teams - 1)),
            dma((chunks, teams - 1)), dma((chunks, teams - 1)),
            dma((chunks, teams)), dma((chunks, teams)),
        ],
        compiler_params=pltpu.CompilerParams(collective_id=0, has_side_effects=True, vmem_limit_bytes=12 << 20),
        name="exchange",
    )(here(presence), owner_of, here(deltas), here(outer_params), here(momentum))
    return pl.pallas_call(
        functools.partial(finish, n),
        out_shape=(
            jax.ShapeDtypeStruct((rows, n * width), bf16),
            jax.ShapeDtypeStruct((rows, width), f32),
            jax.ShapeDtypeStruct((rows, width), f32),
        ),
        in_specs=[smem, vmem, vmem, vmem],
        out_specs=(anywhere, anywhere, anywhere),
        scratch_shapes=[dma((n,)), dma((2,))],
        compiler_params=pltpu.CompilerParams(vmem_limit_bytes=8 << 20),
        name="finish",
    )(owner_of, gathered, outer, speed)


def solution(mesh):
    return jax.shard_map(
        shards,
        mesh=mesh,
        in_specs=(P("rep", "shard", None), P(), P(), P("shard", "rep"), P("shard", "rep")),
        out_specs=(P("shard", None), P("shard", "rep"), P("shard", "rep")),
        check_vma=False,
    )
```

```python
import functools

import jax
import jax.numpy as jnp
from jax import lax
from jax.experimental import pallas as pl
from jax.experimental.pallas import tpu as pltpu
from jax.sharding import PartitionSpec as P

MESH = pl.DeviceIdType.MESH


def toggled(index, mask, size):
    out, bit = 0, 1
    while bit < size:
        digit = (index // bit) % 2
        out = out + bit * ((1 - digit) if mask & bit else digit)
        bit *= 2
    return out


def exchange(n, chunks, presence, owner_of, deltas, outer_params, momentum, gathered, outer_out, momentum_out,
             held_low, held_high, params, speed, out0, in0, out1, own, in1,
             load_sem, state_sem, send0, recv0, send1, recv1, send2, recv2, send3, recv3):
    me = lax.axis_index("rep")
    side, team = me % 2, me // 2
    partner = me + 1 - 2 * side
    teams = n // 2
    rows, width = outer_out.shape
    part = rows // chunks
    mates = [toggled(team, d, teams) for d in range(teams)]
    peers = [2 * mate + side for mate in mates]
    order = list(range(teams - 1, 0, -1))

    def span(k):
        return pl.ds(k * part, part)

    def remote(src, dst, send, recv, to):
        return pltpu.make_async_remote_copy(
            src_ref=src, dst_ref=dst, send_sem=send, recv_sem=recv, device_id={"rep": to}, device_id_type=MESH)

    held = (held_low, held_high)
    pieces, tall = len(held), rows // len(held)
    loads = [[pltpu.make_async_copy(deltas.at[0, pl.ds(i * tall, tall), pl.ds(j * width, width)],
                                    held[i].at[j], load_sem.at[i, j]) for j in range(n)]
             for i in range(pieces)]
    for load in sum(loads, []):
        load.start()
    barrier = pltpu.get_barrier_semaphore()
    for to in [partner] + [peers[d] for d in order]:
        pl.semaphore_signal(barrier, inc=1, device_id={"rep": to}, device_id_type=MESH)

    state = [pltpu.make_async_copy(outer_params, params, state_sem.at[0]),
             pltpu.make_async_copy(momentum, speed, state_sem.at[1])]
    for load in state:
        load.start()

    flag = presence[me].astype(jnp.float32)
    count = presence[0].astype(jnp.float32)
    for r in range(1, n):
        count = count + presence[r].astype(jnp.float32)
    share = jnp.full((1, width), 1.0, jnp.float32) / jnp.full((1, width), count, jnp.float32)

    def term(k, slot):
        piece, first = divmod(k * part, tall)
        return held[piece][owner_of[slot], pl.ds(first, part)].astype(jnp.float32) * flag

    pending = []
    for k in range(chunks):
        if (k * part) % tall == 0:
            for load in loads[k * part // tall]:
                load.wait()
        for d in range(teams):
            out0[k, d] = term(k, 2 * mates[d] + 1 - side).astype(jnp.bfloat16)
        if k == 0:
            pl.semaphore_wait(barrier, teams)
        copy = remote(out0.at[k], in0.at[k], send0.at[k], recv0.at[k], partner)
        copy.start()
        pending.append(copy)
    firsts = list(pending)

    seconds = {}
    for k in range(chunks):
        firsts[k].wait_recv()
        for d in order:
            total = term(k, peers[d]) + in0[k, d].astype(jnp.float32)
            out1[k, d - 1] = total.astype(jnp.bfloat16)
            copy = remote(out1.at[k, d - 1], in1.at[k, d - 1], send1.at[k, d - 1], recv1.at[k, d - 1], peers[d])
            copy.start()
            seconds[k, d] = copy
            pending.append(copy)
        own[span(k)] = term(k, peers[0]) + in0[k, 0].astype(jnp.float32)

    for load in state:
        load.wait()
    thirds, fourths = {}, []
    for k in range(chunks):
        total = own[span(k)]
        for d in order:
            seconds[k, d].wait_recv()
            total = total + in1[k, d - 1].astype(jnp.float32)
        mean = total * share
        new_momentum = 0.9 * speed[span(k)] + mean
        new_outer = params[span(k)] - 0.7 * (mean + 0.9 * new_momentum)
        momentum_out[span(k)] = new_momentum
        outer_out[span(k)] = new_outer
        gathered[me, span(k)] = new_outer.astype(jnp.bfloat16)
        block = gathered.at[me, span(k)]
        for d in order:
            copy = remote(block, block, send2.at[k, d - 1], recv2.at[k, d - 1], peers[d])
            copy.start()
            thirds[k, d] = copy
            pending.append(copy)
        copy = remote(block, block, send3.at[k, 0], recv3.at[k, 0], partner)
        copy.start()
        fourths.append(copy)

    for k in range(chunks):
        for d in order[::-1]:
            thirds[k, d].wait_recv()
            block = gathered.at[peers[d], span(k)]
            copy = remote(block, block, send3.at[k, d], recv3.at[k, d], partner)
            copy.start()
            fourths.append(copy)
    for copy in fourths:
        copy.wait_recv()
    for copy in pending + fourths:
        copy.wait_send()


def finish(n, owner_of, gathered, outer, speed, new_weights, new_outer, new_momentum, block_sem, state_sem):
    width = gathered.shape[2]
    copies = []
    for j in range(n):
        start = pl.multiple_of(owner_of[j] * width, width)
        copies.append(pltpu.make_async_copy(gathered.at[j], new_weights.at[:, pl.ds(start, width)], block_sem.at[j]))
    copies += [pltpu.make_async_copy(outer, new_outer, state_sem.at[0]),
               pltpu.make_async_copy(speed, new_momentum, state_sem.at[1])]
    for copy in copies:
        copy.start()
    for copy in copies:
        copy.wait()


def shards(deltas, presence, owner_of, outer_params, momentum):
    n = lax.axis_size("rep")
    teams = n // 2
    rows, width = outer_params.shape
    chunks = 4
    part = rows // chunks
    bf16, f32 = jnp.bfloat16, jnp.float32
    smem = pl.BlockSpec(memory_space=pltpu.SMEM)
    vmem = pl.BlockSpec(memory_space=pltpu.VMEM)
    anywhere = pl.BlockSpec(memory_space=pl.ANY)
    hbm = pl.BlockSpec(memory_space=pltpu.HBM)
    dma = pltpu.SemaphoreType.DMA
    here = functools.partial(pltpu.with_memory_space_constraint, memory_space=pltpu.HBM)
    owner_of = here(owner_of)
    gathered, outer, speed = pl.pallas_call(
        functools.partial(exchange, n, chunks),
        out_shape=(pltpu.VMEM((n, rows, width), bf16), pltpu.VMEM((rows, width), f32), pltpu.VMEM((rows, width), f32)),
        in_specs=[smem, smem, hbm, hbm, hbm],
        out_specs=(vmem, vmem, vmem),
        scratch_shapes=[
            pltpu.VMEM((n, rows // 2, width), bf16),
            pltpu.VMEM((n, rows // 2, width), bf16),
            pltpu.VMEM((rows, width), f32),
            pltpu.VMEM((rows, width), f32),
            pltpu.VMEM((chunks, teams, part, width), bf16),
            pltpu.VMEM((chunks, teams, part, width), bf16),
            pltpu.VMEM((chunks, teams - 1, part, width), bf16),
            pltpu.VMEM((rows, width), f32),
            pltpu.VMEM((chunks, teams - 1, part, width), bf16),
            dma((2, n)), dma((2,)),
            dma((chunks,)), dma((chunks,)),
            dma((chunks, teams - 1)), dma((chunks, teams - 1)),
            dma((chunks, teams - 1)), dma((chunks, teams - 1)),
            dma((chunks, teams)), dma((chunks, teams)),
        ],
        compiler_params=pltpu.CompilerParams(collective_id=0, has_side_effects=True, vmem_limit_bytes=12 << 20),
        name="exchange",
    )(here(presence), owner_of, here(deltas), here(outer_params), here(momentum))
    return pl.pallas_call(
        functools.partial(finish, n),
        out_shape=(
            jax.ShapeDtypeStruct((rows, n * width), bf16),
            jax.ShapeDtypeStruct((rows, width), f32),
            jax.ShapeDtypeStruct((rows, width), f32),
        ),
        in_specs=[smem, vmem, vmem, vmem],
        out_specs=(anywhere, anywhere, anywhere),
        scratch_shapes=[dma((n,)), dma((2,))],
        compiler_params=pltpu.CompilerParams(vmem_limit_bytes=8 << 20),
        name="finish",
    )(owner_of, gathered, outer, speed)


def solution(mesh):
    return jax.shard_map(
        shards,
        mesh=mesh,
        in_specs=(P("rep", "shard", None), P(), P(), P("shard", "rep"), P("shard", "rep")),
        out_specs=(P("shard", None), P("shard", "rep"), P("shard", "rep")),
        check_vma=False,
    )
```
